32 devices in a mesh: site: 16 (over z, x, core), sec: 2 (over y).
Axes of the slice: x: 2, y: 2, z: 4, core: 2. Of those that a mesh axis runs over, the one named last changes fastest.
Arguments:
- left_canon: bfloat16 [16, 4, 4, 128, 128], P('site', None, 'sec'), may hold values from -1.5 to 1.5
- right_canon: bfloat16 [16, 4, 4, 128, 128], P('site', None, 'sec'), may hold values from -1.5 to 1.5
- center_site: bfloat16 [16, 4, 4, 128, 128], P('site', None, 'sec'), may hold values from -6 to 6
- center_bond: bfloat16 [16, 4, 128, 128], P('site', 'sec'), may hold values from -2 to 3
- left_seed: bfloat16 [16, 4, 128, 128], P('site', 'sec'), may hold values from -2 to 4
- right_seed: bfloat16 [16, 4, 128, 128], P('site', 'sec'), may hold values from -2 to 4
- left_sector: int32 [16, 4, 4], P('site'), may hold values from 0 to 3, each once within a row
- onsite: float32 [16, 4], P('site'), may hold values from 0.5 to 2
- bond_shift: float32 [16], P('site'), may hold values from 0.5 to 2
Outputs:
- left_new: bfloat16 [16, 4, 4, 128, 128], P('site', None, 'sec')
- right_new: bfloat16 [16, 4, 4, 128, 128], P('site', None, 'sec')
The draws below stay inside these ranges and needn't reach their ends.
Inputs may be any that keep to these rules, and one draw needn't show every extreme that they name: `left_sector`: for each site and local state the 4 entries are a permutation of the sectors.
All inputs are finite; a program needn't handle non-finite values.
Results may differ from the reference program's by a relative error of at most 0.028.
Values may be sent and summed in bfloat16 or wider, within the bound.
A program may use at most 64 MiB of HBM per device.

```python
import math
import jax
import jax.numpy as jnp
from jax import lax

B = 128
PHYS = 4
NSI = 10
NAPP = 2
SITES = 16
NSEC = 4
RCH = 4


def noise_shaped(key, shape):
    values = jnp.clip(jax.random.normal(key, shape, jnp.float32), -4.0, 4.0)
    return values


def noise_field(key):
    return noise_shaped(key, (SITES, NSEC, B, B))


def canon_tensor(key):
    values = noise_shaped(jax.random.fold_in(key, 3), (SITES, PHYS, NSEC, B, B))
    leading = jax.random.randint(jax.random.fold_in(key, 5), (SITES,), 0, PHYS)
    states = jnp.arange(PHYS, dtype=jnp.int32)
    weights = jnp.where(states[None, :] == leading[:, None], 0.9, 0.2).astype(jnp.float32)
    identity = jnp.eye(B, dtype=jnp.float32)
    return (weights[:, :, None, None, None] * identity + 0.25 / math.sqrt(B) * values).astype(jnp.bfloat16)


def symmetric_seed(key):
    values = noise_field(jax.random.fold_in(key, 1))
    mixed = (values + jnp.swapaxes(values, -1, -2)) * 0.70710678
    levels = jnp.exp(jax.random.uniform(jax.random.fold_in(key, 2), (SITES, NSEC), jnp.float32, math.log(0.5), math.log(2.0)))
    blocks = jnp.eye(B, dtype=jnp.float32) + 0.5 / math.sqrt(B) * mixed
    return (levels[:, :, None, None] * blocks).astype(jnp.bfloat16)


def draw_left_canon(key, part):
    return canon_tensor(jax.random.fold_in(key, 41))


def draw_right_canon(key, part):
    return canon_tensor(jax.random.fold_in(key, 53))


def draw_center_bond(key, part):
    values = noise_field(jax.random.fold_in(key, 11))
    return (jnp.eye(B, dtype=jnp.float32) + 0.3 / math.sqrt(B) * values).astype(jnp.bfloat16)


def draw_left_seed(key, part):
    return symmetric_seed(jax.random.fold_in(key, 23))


def draw_right_seed(key, part):
    return symmetric_seed(jax.random.fold_in(key, 37))


def shard_levels(key, dims, shards, smallest, largest):
    gain, own = 1.0, jax.random.fold_in(key, 6)
    for position, shards_of in shards:
        draws = jnp.exp(jax.random.uniform(jax.random.fold_in(own, position), (shards_of,), jnp.float32, smallest / len(shards), largest / len(shards)))
        gain = gain * jnp.repeat(draws, dims[position] // shards_of).reshape([-1 if axis == position else 1 for axis in range(len(dims))])
    return gain


def bell_draw(own_key, shape, width, bound, pieces=(), kind=jnp.bfloat16):
    drawn = jax.random.normal(own_key, shape, jnp.float32) * width
    if len(pieces) > 0:
        drawn = shard_levels(own_key, shape, pieces, -0.22, 0.18) * drawn
    return jnp.clip(drawn, min=-bound, max=bound).astype(kind)


def setup_inputs(seed: int = 0) -> dict:
    keys = jax.random.split(jax.random.key(seed), 10)
    left_canon = draw_left_canon(jax.random.fold_in(keys[9], 71), 0)
    right_canon = draw_right_canon(jax.random.fold_in(keys[9], 71), 0)
    center_site = bell_draw(keys[2], (SITES, PHYS, NSEC, B, B), 1.0, 6.0, ((0, 16), (2, 2)))
    center_bond = draw_center_bond(jax.random.fold_in(keys[9], 71), 0)
    left_seed = draw_left_seed(jax.random.fold_in(keys[9], 71), 0)
    right_seed = draw_right_seed(jax.random.fold_in(keys[9], 71), 0)
    left_sector = jax.vmap(lambda own: jax.random.permutation(own, NSEC))(jax.random.split(keys[6], SITES * PHYS)).reshape((SITES, PHYS, NSEC)).astype(jnp.int32)
    onsite = jnp.clip(jnp.exp(math.log(2.0) - 1.3862944 * jax.random.uniform(keys[7], (SITES, PHYS), jnp.float32) ** shard_levels(keys[7], (SITES, PHYS), ((0, 16),), -0.2, 0.2)), 0.5, 2.0)
    bond_shift = jnp.clip(jnp.exp(math.log(2.0) - 1.3862944 * jax.random.uniform(keys[8], (SITES,), jnp.float32) ** shard_levels(keys[8], (SITES,), ((0, 16),), -0.2, 0.2)), 0.5, 2.0)
    return {"left_canon": left_canon, "right_canon": right_canon, "center_site": center_site, "center_bond": center_bond, "left_seed": left_seed, "right_seed": right_seed, "left_sector": left_sector, "onsite": onsite, "bond_shift": bond_shift}


def pick_blocks(blocks, indices):
    return jax.vmap(lambda chosen, where_at: jnp.take(chosen, where_at, axis=0))(blocks, indices)

def inverse_root(gram_mat):
    scaling = jnp.sqrt(lax.optimization_barrier(jnp.sum(gram_mat * gram_mat, axis=(-2, -1), keepdims=True)))
    identity = jnp.eye(gram_mat.shape[-1], dtype=jnp.float32)
    upper_part = gram_mat / scaling
    lower_part = jnp.broadcast_to(identity, gram_mat.shape)
    for repeat in range(NSI):
        middle = 1.5 * identity - 0.5 * jnp.matmul(lower_part, upper_part, precision=lax.Precision.HIGHEST)
        upper_part = jnp.matmul(upper_part, middle, precision=lax.Precision.HIGHEST)
        lower_part = jnp.matmul(middle, lower_part, precision=lax.Precision.HIGHEST)
    return lower_part / jnp.sqrt(scaling)

def trace_sum(blocks):
    return lax.optimization_barrier(jnp.sum(jnp.diagonal(blocks.astype(jnp.float32), axis1=2, axis2=3), axis=(1, 2)))

def reference(left_canon, right_canon, center_site, center_bond, left_seed, right_seed, left_sector, onsite, bond_shift):
    labels = jnp.arange(NSEC, dtype=jnp.int32)
    right_of = lax.optimization_barrier(jnp.sum(jnp.where(left_sector[:, :, :, None] == labels[None, None, None, :], labels[None, None, :, None], 0), axis=2)).astype(jnp.int32)
    routing = (left_sector[:, :, :, None] == labels[None, None, None, :]).astype(jnp.float32)

    def left_step(hold):
        running = jnp.zeros(hold.shape, jnp.float32)
        for physical in range(PHYS):
            tensor = left_canon[:, physical].astype(jnp.float32)
            chosen = pick_blocks(hold, left_sector[:, physical]).astype(jnp.float32)
            product = jnp.einsum('jkab,jkbc->jkac', chosen, tensor).astype(jnp.bfloat16)
            running = running + jnp.einsum('jkba,jkbc->jkac', tensor, product.astype(jnp.float32))
        return running.astype(jnp.bfloat16)

    def right_step(hold):
        running = jnp.zeros(hold.shape, jnp.float32)
        for physical in range(PHYS):
            picked = pick_blocks(right_canon[:, physical], right_of[:, physical]).astype(jnp.float32)
            env_chosen = pick_blocks(hold, right_of[:, physical]).astype(jnp.float32)
            product = jnp.einsum('jkab,jkbc->jkac', picked, env_chosen).astype(jnp.bfloat16)
            running = running + jnp.einsum('jkac,jkdc->jkad', product.astype(jnp.float32), picked)
        return running.astype(jnp.bfloat16)
    left_hold = left_seed
    right_hold = right_seed
    left_fresh = left_seed
    for step in range(RCH):
        left_fresh = left_step(left_hold)
        right_fresh = right_step(right_hold)
        left_hold = jnp.roll(left_fresh, 1, axis=0)
        right_hold = jnp.roll(right_fresh, -1, axis=0)
    dim_all = NSEC * B

    def scaled(blocks):
        return (blocks.astype(jnp.float32) * (dim_all / trace_sum(blocks))[:, None, None, None]).astype(jnp.bfloat16)
    cur_scaled = scaled(left_hold)
    next_scaled = scaled(left_fresh)
    right_scaled = scaled(right_hold)
    chosen_left = pick_blocks(cur_scaled, left_sector).astype(jnp.float32)
    site_now = center_site
    bond_now = center_bond
    for repeat in range(NAPP):
        half_site = jnp.einsum('jskab,jskbc->jskac', chosen_left, site_now.astype(jnp.float32)).astype(jnp.bfloat16)
        site_now = (jnp.einsum('jskab,jkbc->jskac', half_site.astype(jnp.float32), right_scaled.astype(jnp.float32)) + onsite[:, :, None, None, None] * site_now.astype(jnp.float32)).astype(jnp.bfloat16)
        half_bond = jnp.einsum('jkab,jkbc->jkac', next_scaled.astype(jnp.float32), bond_now.astype(jnp.float32)).astype(jnp.bfloat16)
        bond_now = (jnp.einsum('jkab,jkbc->jkac', half_bond.astype(jnp.float32), right_scaled.astype(jnp.float32)) + bond_shift[:, None, None, None] * bond_now.astype(jnp.float32)).astype(jnp.bfloat16)
    site_wide = site_now.astype(jnp.float32)
    bond_wide = bond_now.astype(jnp.float32)
    gram_left = jnp.einsum('jskab,jskac->jkbc', site_wide, site_wide)
    gram_bond = jnp.einsum('jkab,jkac->jkbc', bond_wide, bond_wide)
    unit_left = jnp.matmul(bond_wide, inverse_root(gram_bond), precision=lax.Precision.HIGHEST)
    factor_left = jnp.matmul(inverse_root(gram_left), jnp.swapaxes(unit_left, -1, -2), precision=lax.Precision.HIGHEST).astype(jnp.bfloat16)
    left_new = jnp.einsum('jskab,jkbc->jskac', site_wide, factor_left.astype(jnp.float32)).astype(jnp.bfloat16)
    outer_terms = jnp.einsum('jskab,jskcb->jskac', site_wide, site_wide)
    gram_right = jnp.einsum('jskm,jskac->jmac', routing, outer_terms)
    previous = jnp.roll(bond_now, 1, axis=0).astype(jnp.float32)
    gram_prev = jnp.matmul(previous, jnp.swapaxes(previous, -1, -2), precision=lax.Precision.HIGHEST)
    unit_right = jnp.matmul(inverse_root(gram_prev), previous, precision=lax.Precision.HIGHEST)
    factor_right = jnp.matmul(jnp.swapaxes(unit_right, -1, -2), inverse_root(gram_right), precision=lax.Precision.HIGHEST).astype(jnp.bfloat16)
    factor_chosen = pick_blocks(factor_right, left_sector).astype(jnp.float32)
    right_new = jnp.einsum('jskab,jskbc->jskac', factor_chosen, site_wide).astype(jnp.bfloat16)
    return (left_new, right_new)
```

```python
import functools

import jax
import jax.numpy as jnp
from jax import lax
from jax.experimental import pallas as pl
from jax.experimental.pallas import tpu as pltpu
from jax.sharding import PartitionSpec as P

NSI = 10
NAPP = 2
MESH = pl.DeviceIdType.MESH
F32 = jnp.float32
BF16 = jnp.bfloat16


def dot(a, b):
    return lax.dot_general(a, b, (((1,), (0,)), ((), ())), preferred_element_type=F32)


def dot_nt(a, b):
    return lax.dot_general(a, b, (((1,), (1,)), ((), ())), preferred_element_type=F32)


def dot_tn(a, b):
    return lax.dot_general(a, b, (((0,), (0,)), ((), ())), preferred_element_type=F32)


def split(x):
    hi = x.astype(BF16)
    return hi, (x - hi.astype(F32)).astype(BF16)


def as_lhs(pair):
    return jnp.concatenate(pair, axis=1)


def as_rhs(pair):
    row = jnp.concatenate(pair, axis=1)
    return jnp.concatenate((row, row), axis=0)


def mm(lhs_pair, rhs_pair):
    out = dot(as_lhs(lhs_pair), as_rhs(rhs_pair))
    width = out.shape[1] // 2
    return out[:, :width] + out[:, width:]


def kernel(
    steps, sites, parts, phys, owned,
    lc, rc, cs, cb, lseed, rseed, src, onsite, shift,
    left_new, right_new,
    hold_l, lrecv, lsend, rrecv, psend, terms, lct, site, bond, ys, zs, env_r, env_n,
    gsend, grecv, usend, urecv, fsend, frecv, fall, tns, tnr, trs, trr,
    s_ls, s_lr, s_ps, s_pr, s_gs, s_gr, s_us, s_ur, s_fs, s_fr, s_tns, s_tnr, s_trs, s_trr,
):
    j = lax.axis_index("site")
    me = lax.axis_index("sec")
    after, before = lax.rem(j + 1, sites), lax.rem(j + sites - 1, sites)
    off = me * owned
    width = lc.shape[-1]
    sectors = parts * owned

    def sec(d):
        return lax.rem(me + d, parts)

    def copy(a, b, ss, rs, to_site, to_sec):
        return pltpu.make_async_remote_copy(
            src_ref=a, dst_ref=b, send_sem=ss, recv_sem=rs,
            device_id={"site": to_site, "sec": to_sec}, device_id_type=MESH,
        )

    def c_seed(d):
        return copy(lseed.at[0], lrecv.at[0, me], s_ls.at[steps, d], s_lr.at[0, me], j, sec(d))

    def c_left(t, d):
        return copy(lsend.at[t], lrecv.at[t + 1, me], s_ls.at[t, d], s_lr.at[t + 1, me], after, sec(d))

    def c_right(t, d):
        return copy(psend.at[t, d], rrecv.at[t, me], s_ps.at[t, d], s_pr.at[t, me], before, sec(d))

    def c_tn(d):
        return copy(tns, tnr.at[me], s_tns.at[d], s_tnr.at[me], j, sec(d))

    def c_tr(d):
        return copy(trs, trr.at[me], s_trs.at[d], s_trr.at[me], before, sec(d))

    def c_gram(d):
        return copy(gsend.at[d], grecv.at[me], s_gs.at[d], s_gr.at[me], j, sec(d))

    def c_unit():
        return copy(usend, urecv, s_us.at[0], s_ur.at[0], after, me)

    def c_factor(d):
        return copy(fsend, frecv.at[me], s_fs.at[d], s_fr.at[me], j, sec(d))

    def got(ref, sem):
        copy(ref, ref, s_us.at[0], sem, after, me).wait_recv()

    barrier = pltpu.get_barrier_semaphore()
    for d in range(parts):
        for where in (after, before) if d == 0 else (after, before, j):
            pl.semaphore_signal(
                barrier, inc=1, device_id={"site": where, "sec": sec(d)}, device_id_type=MESH
            )
    pl.semaphore_wait(barrier, 3 * parts - 1)

    for d in range(1, parts):
        c_seed(d).start()

    sources = [[src[0, s, off + k] for k in range(owned)] for s in range(phys)]

    def gathered(target, i):
        want = target * owned + i
        total = None
        for s in range(phys):
            hit, at = jnp.int32(0), jnp.int32(0)
            for k in range(owned):
                same = (sources[s][k] == want).astype(jnp.int32)
                hit, at = hit + same, at + same * k
            term = terms[s * owned + at] * hit.astype(F32)
            total = term if total is None else total + term
        return total

    for k in range(owned):
        for s in range(phys):
            lct[k, :, s * width : (s + 1) * width] = lc[0, s, k].T
    for k in range(owned):
        env_r[k] = rseed[0, k]
        hold_l[off + k] = lseed[0, k]
    for d in range(1, parts):
        a = sec(d)
        got(lrecv.at[0, a], s_lr.at[0, a])
        for k in range(owned):
            hold_l[a * owned + k] = lrecv[0, a, k]

    def left_arrival(t):
        for d in range(parts):
            a = sec(d)
            got(lrecv.at[t, a], s_lr.at[t, a])
            for k in range(owned):
                hold_l[a * owned + k] = lrecv[t, a, k]

    def right_arrival(t):
        for d in range(parts):
            a = sec(d)
            got(rrecv.at[t, a], s_pr.at[t, a])
        for k in range(owned):
            total = rrecv[t, 0, k].astype(F32)
            for a in range(1, parts):
                total = total + rrecv[t, a, k].astype(F32)
            env_r[k] = total.astype(BF16)

    def turn(t, carry):
        for k in range(owned):
            prods = [
                dot(hold_l[sources[s][k]], lc[0, s, k]).astype(BF16) for s in range(phys)
            ]
            lsend[t, k] = dot(lct[k], jnp.concatenate(prods, axis=0)).astype(BF16)
        for d in range(parts):
            c_left(t, d).start()

        @pl.when(t > 0)
        def _():
            right_arrival(t - 1)

        for k in range(owned):
            stack = jnp.concatenate([rc[0, s, k] for s in range(phys)], axis=0)
            prod = dot(stack, env_r[k]).astype(BF16)
            for s in range(phys):
                terms[s * owned + k] = dot_nt(prod[s * width : (s + 1) * width], rc[0, s, k])
        for d in range(parts):
            for i in range(owned):
                psend[t, d, i] = gathered(sec(d), i).astype(BF16)
            c_right(t, d).start()

        @pl.when(t < steps - 1)
        def _():
            left_arrival(t + 1)

        return carry

    lax.fori_loop(0, steps, turn, 0)

    rows = lax.broadcasted_iota(jnp.int32, (width, width), 0)
    cols = lax.broadcasted_iota(jnp.int32, (width, width), 1)
    diagonal = (rows == cols).astype(F32)

    def traces(blocks):
        total = None
        for block in blocks:
            total = block.astype(F32) if total is None else total + block.astype(F32)
        return jnp.sum((total * diagonal).reshape(width // 8, 8, width), axis=0)

    tns[...] = traces([lsend[steps - 1, k] for k in range(owned)])
    for d in range(1, parts):
        c_tn(d).start()
    trs[...] = traces([psend[steps - 1, d, i] for d in range(parts) for i in range(owned)])
    for d in range(parts):
        c_tr(d).start()

    def scale_of(total):
        return (sectors * width) / jnp.sum(total, axis=(0, 1), keepdims=True)

    total = tns[...]
    for d in range(1, parts):
        a = sec(d)
        got(tnr.at[a], s_tnr.at[a])
        total = total + tnr[a]
    scale = scale_of(total)
    for k in range(owned):
        env_n[k] = (lsend[steps - 1, k].astype(F32) * scale).astype(BF16)

    left_arrival(steps)
    scale = scale_of(traces([hold_l[m] for m in range(sectors)]))
    for m in range(sectors):
        hold_l[m] = (hold_l[m].astype(F32) * scale).astype(BF16)

    right_arrival(steps - 1)
    for a in range(parts):
        got(trr.at[a], s_trr.at[a])
    total = trr[0]
    for a in range(1, parts):
        total = total + trr[a]
    scale = scale_of(total)
    for k in range(owned):
        env_r[k] = (env_r[k].astype(F32) * scale).astype(BF16)

    for k in range(owned):
        for s in range(phys):
            site[k, s * width : (s + 1) * width] = cs[0, s, k]
        bond[k] = cb[0, k]
    for repeat in range(NAPP):
        for k in range(owned):
            halves = [
                dot(hold_l[sources[s][k]], site[k, s * width : (s + 1) * width]).astype(BF16)
                for s in range(phys)
            ]
            whole = dot(jnp.concatenate(halves, axis=0), env_r[k])
            for s in range(phys):
                part = slice(s * width, (s + 1) * width)
                site[k, part] = (whole[part] + onsite[0, s] * site[k, part].astype(F32)).astype(BF16)

    for k in range(owned):
        for s in range(phys):
            block = site[k, s * width : (s + 1) * width]
            terms[s * owned + k] = dot_nt(block, block)
    for d in range(parts - 1, -1, -1):
        for i in range(owned):
            gsend[d, i] = gathered(sec(d), i)
        if d > 0:
            c_gram(d).start()

    for repeat in range(NAPP):
        for k in range(owned):
            half = dot(env_n[k], bond[k]).astype(BF16)
            bond[k] = (dot(half, env_r[k]) + shift[0] * bond[k].astype(F32)).astype(BF16)

    def inverse_roots(grams):
        norms = []
        for i, gram in enumerate(grams):
            norm = jnp.sqrt(jnp.sum(gram * gram, axis=(0, 1), keepdims=True))
            norms.append(norm)
            upper = gram / norm
            middle = 1.5 * diagonal - 0.5 * upper
            ys[i] = mm(split(upper), split(middle))
            zs[i] = middle

        def body(n, carry):
            uppers = [split(ys[i]) for i in range(len(grams))]
            lowers = [split(zs[i]) for i in range(len(grams))]
            middles = [
                split(1.5 * diagonal - 0.5 * mm(z, y)) for z, y in zip(lowers, uppers)
            ]
            for i in range(len(grams)):
                ys[i] = mm(uppers[i], middles[i])
                zs[i] = mm(middles[i], lowers[i])
            return carry

        lax.fori_loop(0, NSI - 2, body, 0)
        for i in range(len(grams)):
            lower = split(zs[i])
            middle = split(1.5 * diagonal - 0.5 * mm(lower, split(ys[i])))
            zs[i] = mm(middle, lower) / jnp.sqrt(norms[i])

    inverse_roots(
        [dot_tn(bond[k], bond[k]) for k in range(owned)]
        + [dot_tn(site[k], site[k]) for k in range(owned)]
    )
    factors = []
    for k in range(owned):
        hi, lo = split(zs[k])
        unit_t = dot_nt(hi, bond[k]) + dot_nt(lo, bond[k])
        usend[k] = unit_t.astype(BF16)
        factors.append(mm(split(zs[owned + k]), split(unit_t)).astype(BF16))
    c_unit().start()

    for d in range(1, parts):
        a = sec(d)
        got(grecv.at[a], s_gr.at[a])
    grams = []
    for i in range(owned):
        total = gsend[0, i]
        for d in range(1, parts):
            total = total + grecv[sec(d), i]
        grams.append(total)
    inverse_roots(grams)
    got(urecv, s_ur.at[0])
    for i in range(owned):
        hi, lo = split(zs[i])
        fsend[i] = (dot(urecv[i], hi) + dot(urecv[i], lo)).astype(BF16)
    for d in range(1, parts):
        c_factor(d).start()

    for k in range(owned):
        whole = dot(site[k], factors[k]).astype(BF16)
        for s in range(phys):
            left_new[0, s, k] = whole[s * width : (s + 1) * width]
    for i in range(owned):
        fall[off + i] = fsend[i]
    for d in range(1, parts):
        a = sec(d)
        got(frecv.at[a], s_fr.at[a])
        for i in range(owned):
            fall[a * owned + i] = frecv[a, i]
    for k in range(owned):
        for s in range(phys):
            block = site[k, s * width : (s + 1) * width]
            right_new[0, s, k] = dot(fall[sources[s][k]], block).astype(BF16)

    def drain(t, carry):
        for d in range(parts):
            c_left(t, d).wait_send()
            c_right(t, d).wait_send()
        return carry

    lax.fori_loop(0, steps, drain, 0)
    for d in range(parts):
        c_tr(d).wait_send()
    for d in range(1, parts):
        for c in (c_seed, c_tn, c_gram, c_factor):
            c(d).wait_send()
    c_unit().wait_send()


def per_device(lc, rc, cs, cb, lseed, rseed, src, onsite, shift):
    sites, parts = lax.axis_size("site"), lax.axis_size("sec")
    steps = sites // 4
    _, phys, owned, width, _ = lc.shape
    sectors = parts * owned
    block = (width, width)
    most = 2 * owned

    def vm(*shape, dtype=BF16):
        return pltpu.VMEM(shape, dtype)

    def dma(*shape):
        return pltpu.SemaphoreType.DMA(shape)

    in_vmem = pl.BlockSpec(memory_space=pltpu.VMEM)
    in_smem = pl.BlockSpec(memory_space=pltpu.SMEM)
    shape = jax.ShapeDtypeStruct(cs.shape, BF16)
    return pl.pallas_call(
        functools.partial(kernel, steps, sites, parts, phys, owned),
        out_shape=(shape, shape),
        in_specs=[in_vmem] * 6 + [in_smem] * 3,
        out_specs=(in_vmem, in_vmem),
        scratch_shapes=[
            vm(sectors, *block),
            vm(steps + 1, parts, owned, *block),
            vm(steps, owned, *block),
            vm(steps, parts, owned, *block),
            vm(steps, parts, owned, *block),
            vm(phys * owned, *block, dtype=F32),
            vm(owned, width, phys * width),
            vm(owned, phys * width, width),
            vm(owned, *block),
            vm(most, *block, dtype=F32),
            vm(most, *block, dtype=F32),
            vm(owned, *block),
            vm(owned, *block),
            vm(parts, owned, *block, dtype=F32),
            vm(parts, owned, *block, dtype=F32),
            vm(owned, *block),
            vm(owned, *block),
            vm(owned, *block),
            vm(parts, owned, *block),
            vm(sectors, *block),
            vm(8, width, dtype=F32),
            vm(parts, 8, width, dtype=F32),
            vm(8, width, dtype=F32),
            vm(parts, 8, width, dtype=F32),
            dma(steps + 1, parts), dma(steps + 1, parts),
            dma(steps, parts), dma(steps, parts),
            dma(parts), dma(parts),
            dma(1), dma(1),
            dma(parts), dma(parts),
            dma(parts), dma(parts),
            dma(parts), dma(parts),
        ],
        compiler_params=pltpu.CompilerParams(
            collective_id=0, has_side_effects=True, vmem_limit_bytes=60 * 1024 * 1024
        ),
    )(lc, rc, cs, cb, lseed, rseed, src, onsite, shift)


def solution(mesh):
    tensor = P("site", None, "sec", None, None)
    blocks = P("site", "sec", None, None)
    return jax.shard_map(
        per_device,
        mesh=mesh,
        in_specs=(tensor, tensor, tensor, blocks, blocks, blocks,
                  P("site", None, None), P("site", None), P("site")),
        out_specs=(tensor, tensor),
        check_vma=False,
    )
```

```python
import functools

import jax
import jax.numpy as jnp
from jax import lax
from jax.experimental import pallas as pl
from jax.experimental.pallas import tpu as pltpu
from jax.sharding import PartitionSpec as P

NSI = 10
NAPP = 2
MESH = pl.DeviceIdType.MESH
F32 = jnp.float32
BF16 = jnp.bfloat16


def dot(a, b):
    return lax.dot_general(a, b, (((1,), (0,)), ((), ())), preferred_element_type=F32)


def dot_nt(a, b):
    return lax.dot_general(a, b, (((1,), (1,)), ((), ())), preferred_element_type=F32)


def dot_tn(a, b):
    return lax.dot_general(a, b, (((0,), (0,)), ((), ())), preferred_element_type=F32)


def split(x):
    hi = x.astype(BF16)
    return hi, (x - hi.astype(F32)).astype(BF16)


def as_lhs(pair):
    return jnp.concatenate(pair, axis=1)


def as_rhs(pair):
    row = jnp.concatenate(pair, axis=1)
    return jnp.concatenate((row, row), axis=0)


def mm(lhs_pair, rhs_pair):
    out = dot(as_lhs(lhs_pair), as_rhs(rhs_pair))
    width = out.shape[1] // 2
    return out[:, :width] + out[:, width:]


def kernel(
    steps, sites, parts, phys, owned,
    lc, rc, cs, cb, lseed, rseed, src, onsite, shift,
    left_new, right_new,
    hold_l, lrecv, lsend, rrecv, psend, terms, lct, site, bond, ys, zs, env_r, env_n,
    gsend, grecv, usend, urecv, fsend, frecv, fall, tns, tnr, trs, trr,
    s_ls, s_lr, s_ps, s_pr, s_gs, s_gr, s_us, s_ur, s_fs, s_fr, s_tns, s_tnr, s_trs, s_trr,
):
    j = lax.axis_index("site")
    me = lax.axis_index("sec")
    after, before = lax.rem(j + 1, sites), lax.rem(j + sites - 1, sites)
    off = me * owned
    width = lc.shape[-1]
    sectors = parts * owned

    def sec(d):
        return lax.rem(me + d, parts)

    def copy(a, b, ss, rs, to_site, to_sec):
        return pltpu.make_async_remote_copy(
            src_ref=a, dst_ref=b, send_sem=ss, recv_sem=rs,
            device_id={"site": to_site, "sec": to_sec}, device_id_type=MESH,
        )

    def c_seed(d):
        return copy(lseed.at[0], lrecv.at[0, me], s_ls.at[steps, d], s_lr.at[0, me], j, sec(d))

    def c_left(t, d):
        return copy(lsend.at[t], lrecv.at[t + 1, me], s_ls.at[t, d], s_lr.at[t + 1, me], after, sec(d))

    def c_right(t, d):
        return copy(psend.at[t, d], rrecv.at[t, me], s_ps.at[t, d], s_pr.at[t, me], before, sec(d))

    def c_tn(d):
        return copy(tns, tnr.at[me], s_tns.at[d], s_tnr.at[me], j, sec(d))

    def c_tr(d):
        return copy(trs, trr.at[me], s_trs.at[d], s_trr.at[me], before, sec(d))

    def c_gram(d):
        return copy(gsend.at[d], grecv.at[me], s_gs.at[d], s_gr.at[me], j, sec(d))

    def c_unit():
        return copy(usend, urecv, s_us.at[0], s_ur.at[0], after, me)

    def c_factor(d):
        return copy(fsend, frecv.at[me], s_fs.at[d], s_fr.at[me], j, sec(d))

    def got(ref, sem):
        copy(ref, ref, s_us.at[0], sem, after, me).wait_recv()

    barrier = pltpu.get_barrier_semaphore()
    for d in range(parts):
        for where in (after, before) if d == 0 else (after, before, j):
            pl.semaphore_signal(
                barrier, inc=1, device_id={"site": where, "sec": sec(d)}, device_id_type=MESH
            )
    pl.semaphore_wait(barrier, 3 * parts - 1)

    for d in range(1, parts):
        c_seed(d).start()

    sources = [[src[0, s, off + k] for k in range(owned)] for s in range(phys)]

    def gathered(target, i):
        want = target * owned + i
        total = None
        for s in range(phys):
            hit, at = jnp.int32(0), jnp.int32(0)
            for k in range(owned):
                same = (sources[s][k] == want).astype(jnp.int32)
                hit, at = hit + same, at + same * k
            term = terms[s * owned + at] * hit.astype(F32)
            total = term if total is None else total + term
        return total

    for k in range(owned):
        for s in range(phys):
            lct[k, :, s * width : (s + 1) * width] = lc[0, s, k].T
    for k in range(owned):
        env_r[k] = rseed[0, k]
        hold_l[off + k] = lseed[0, k]
    def seed_arrival():
        for d in range(1, parts):
            a = sec(d)
            got(lrecv.at[0, a], s_lr.at[0, a])
            for k in range(owned):
                hold_l[a * owned + k] = lrecv[0, a, k]

    def left_arrival(t):
        for d in range(parts):
            a = sec(d)
            got(lrecv.at[t, a], s_lr.at[t, a])
            for k in range(owned):
                hold_l[a * owned + k] = lrecv[t, a, k]

    def right_arrival(t):
        for d in range(parts):
            a = sec(d)
            got(rrecv.at[t, a], s_pr.at[t, a])
        for k in range(owned):
            total = rrecv[t, 0, k].astype(F32)
            for a in range(1, parts):
                total = total + rrecv[t, a, k].astype(F32)
            env_r[k] = total.astype(BF16)

    def turn(t, carry):
        @pl.when(t > 0)
        def _():
            right_arrival(t - 1)

        for k in range(owned):
            stack = jnp.concatenate([rc[0, s, k] for s in range(phys)], axis=0)
            prod = dot(stack, env_r[k]).astype(BF16)
            for s in range(phys):
                terms[s * owned + k] = dot_nt(prod[s * width : (s + 1) * width], rc[0, s, k])
        for d in range(parts):
            for i in range(owned):
                psend[t, d, i] = gathered(sec(d), i).astype(BF16)
            c_right(t, d).start()

        @pl.when(t == 0)
        def _():
            seed_arrival()

        @pl.when(t > 0)
        def _():
            left_arrival(t)

        for k in range(owned):
            prods = [
                dot(hold_l[sources[s][k]], lc[0, s, k]).astype(BF16) for s in range(phys)
            ]
            lsend[t, k] = dot(lct[k], jnp.concatenate(prods, axis=0)).astype(BF16)
        for d in range(parts):
            c_left(t, d).start()

        return carry

    lax.fori_loop(0, steps, turn, 0)

    rows = lax.broadcasted_iota(jnp.int32, (width, width), 0)
    cols = lax.broadcasted_iota(jnp.int32, (width, width), 1)
    diagonal = (rows == cols).astype(F32)

    def traces(blocks):
        total = None
        for block in blocks:
            total = block.astype(F32) if total is None else total + block.astype(F32)
        return jnp.sum((total * diagonal).reshape(width // 8, 8, width), axis=0)

    tns[...] = traces([lsend[steps - 1, k] for k in range(owned)])
    for d in range(1, parts):
        c_tn(d).start()
    trs[...] = traces([psend[steps - 1, d, i] for d in range(parts) for i in range(owned)])
    for d in range(parts):
        c_tr(d).start()

    def scale_of(total):
        return (sectors * width) / jnp.sum(total, axis=(0, 1), keepdims=True)

    total = tns[...]
    for d in range(1, parts):
        a = sec(d)
        got(tnr.at[a], s_tnr.at[a])
        total = total + tnr[a]
    scale = scale_of(total)
    for k in range(owned):
        env_n[k] = (lsend[steps - 1, k].astype(F32) * scale).astype(BF16)

    left_arrival(steps)
    scale = scale_of(traces([hold_l[m] for m in range(sectors)]))
    for m in range(sectors):
        hold_l[m] = (hold_l[m].astype(F32) * scale).astype(BF16)

    right_arrival(steps - 1)
    for a in range(parts):
        got(trr.at[a], s_trr.at[a])
    total = trr[0]
    for a in range(1, parts):
        total = total + trr[a]
    scale = scale_of(total)
    for k in range(owned):
        env_r[k] = (env_r[k].astype(F32) * scale).astype(BF16)

    for k in range(owned):
        for s in range(phys):
            site[k, s * width : (s + 1) * width] = cs[0, s, k]
        bond[k] = cb[0, k]
    for repeat in range(NAPP):
        for k in range(owned):
            halves = [
                dot(hold_l[sources[s][k]], site[k, s * width : (s + 1) * width]).astype(BF16)
                for s in range(phys)
            ]
            whole = dot(jnp.concatenate(halves, axis=0), env_r[k])
            for s in range(phys):
                part = slice(s * width, (s + 1) * width)
                site[k, part] = (whole[part] + onsite[0, s] * site[k, part].astype(F32)).astype(BF16)

    for k in range(owned):
        for s in range(phys):
            block = site[k, s * width : (s + 1) * width]
            terms[s * owned + k] = dot_nt(block, block)
    for d in range(parts - 1, -1, -1):
        for i in range(owned):
            gsend[d, i] = gathered(sec(d), i)
        if d > 0:
            c_gram(d).start()

    for repeat in range(NAPP):
        for k in range(owned):
            half = dot(env_n[k], bond[k]).astype(BF16)
            bond[k] = (dot(half, env_r[k]) + shift[0] * bond[k].astype(F32)).astype(BF16)

    def inverse_roots(grams):
        norms = []
        for i, gram in enumerate(grams):
            norm = jnp.sqrt(jnp.sum(gram * gram, axis=(0, 1), keepdims=True))
            norms.append(norm)
            upper = gram / norm
            middle = 1.5 * diagonal - 0.5 * upper
            ys[i] = mm(split(upper), split(middle))
            zs[i] = middle

        def body(n, carry):
            uppers = [split(ys[i]) for i in range(len(grams))]
            lowers = [split(zs[i]) for i in range(len(grams))]
            middles = [
                split(1.5 * diagonal - 0.5 * mm(z, y)) for z, y in zip(lowers, uppers)
            ]
            for i in range(len(grams)):
                ys[i] = mm(uppers[i], middles[i])
                zs[i] = mm(middles[i], lowers[i])
            return carry

        lax.fori_loop(0, NSI - 2, body, 0)
        for i in range(len(grams)):
            lower = split(zs[i])
            middle = split(1.5 * diagonal - 0.5 * mm(lower, split(ys[i])))
            zs[i] = mm(middle, lower) / jnp.sqrt(norms[i])

    inverse_roots(
        [dot_tn(bond[k], bond[k]) for k in range(owned)]
        + [dot_tn(site[k], site[k]) for k in range(owned)]
    )
    factors = []
    for k in range(owned):
        hi, lo = split(zs[k])
        unit_t = dot_nt(hi, bond[k]) + dot_nt(lo, bond[k])
        usend[k] = unit_t.astype(BF16)
        factors.append(mm(split(zs[owned + k]), split(unit_t)).astype(BF16))
    c_unit().start()

    for d in range(1, parts):
        a = sec(d)
        got(grecv.at[a], s_gr.at[a])
    grams = []
    for i in range(owned):
        total = gsend[0, i]
        for d in range(1, parts):
            total = total + grecv[sec(d), i]
        grams.append(total)
    inverse_roots(grams)
    got(urecv, s_ur.at[0])
    for i in range(owned):
        hi, lo = split(zs[i])
        fsend[i] = (dot(urecv[i], hi) + dot(urecv[i], lo)).astype(BF16)
    for d in range(1, parts):
        c_factor(d).start()

    for k in range(owned):
        whole = dot(site[k], factors[k]).astype(BF16)
        for s in range(phys):
            left_new[0, s, k] = whole[s * width : (s + 1) * width]
    for i in range(owned):
        fall[off + i] = fsend[i]
    for d in range(1, parts):
        a = sec(d)
        got(frecv.at[a], s_fr.at[a])
        for i in range(owned):
            fall[a * owned + i] = frecv[a, i]
    for k in range(owned):
        for s in range(phys):
            block = site[k, s * width : (s + 1) * width]
            right_new[0, s, k] = dot(fall[sources[s][k]], block).astype(BF16)

    def drain(t, carry):
        for d in range(parts):
            c_left(t, d).wait_send()
            c_right(t, d).wait_send()
        return carry

    lax.fori_loop(0, steps, drain, 0)
    for d in range(parts):
        c_tr(d).wait_send()
    for d in range(1, parts):
        for c in (c_seed, c_tn, c_gram, c_factor):
            c(d).wait_send()
    c_unit().wait_send()


def per_device(lc, rc, cs, cb, lseed, rseed, src, onsite, shift):
    sites, parts = lax.axis_size("site"), lax.axis_size("sec")
    steps = sites // 4
    _, phys, owned, width, _ = lc.shape
    sectors = parts * owned
    block = (width, width)
    most = 2 * owned

    def vm(*shape, dtype=BF16):
        return pltpu.VMEM(shape, dtype)

    def dma(*shape):
        return pltpu.SemaphoreType.DMA(shape)

    in_vmem = pl.BlockSpec(memory_space=pltpu.VMEM)
    in_smem = pl.BlockSpec(memory_space=pltpu.SMEM)
    shape = jax.ShapeDtypeStruct(cs.shape, BF16)
    return pl.pallas_call(
        functools.partial(kernel, steps, sites, parts, phys, owned),
        out_shape=(shape, shape),
        in_specs=[in_vmem] * 6 + [in_smem] * 3,
        out_specs=(in_vmem, in_vmem),
        scratch_shapes=[
            vm(sectors, *block),
            vm(steps + 1, parts, owned, *block),
            vm(steps, owned, *block),
            vm(steps, parts, owned, *block),
            vm(steps, parts, owned, *block),
            vm(phys * owned, *block, dtype=F32),
            vm(owned, width, phys * width),
            vm(owned, phys * width, width),
            vm(owned, *block),
            vm(most, *block, dtype=F32),
            vm(most, *block, dtype=F32),
            vm(owned, *block),
            vm(owned, *block),
            vm(parts, owned, *block, dtype=F32),
            vm(parts, owned, *block, dtype=F32),
            vm(owned, *block),
            vm(owned, *block),
            vm(owned, *block),
            vm(parts, owned, *block),
            vm(sectors, *block),
            vm(8, width, dtype=F32),
            vm(parts, 8, width, dtype=F32),
            vm(8, width, dtype=F32),
            vm(parts, 8, width, dtype=F32),
            dma(steps + 1, parts), dma(steps + 1, parts),
            dma(steps, parts), dma(steps, parts),
            dma(parts), dma(parts),
            dma(1), dma(1),
            dma(parts), dma(parts),
            dma(parts), dma(parts),
            dma(parts), dma(parts),
        ],
        compiler_params=pltpu.CompilerParams(
            collective_id=0, has_side_effects=True, vmem_limit_bytes=60 * 1024 * 1024
        ),
    )(lc, rc, cs, cb, lseed, rseed, src, onsite, shift)


def solution(mesh):
    tensor = P("site", None, "sec", None, None)
    blocks = P("site", "sec", None, None)
    return jax.shard_map(
        per_device,
        mesh=mesh,
        in_specs=(tensor, tensor, tensor, blocks, blocks, blocks,
                  P("site", None, None), P("site", None), P("site")),
        out_specs=(tensor, tensor),
        check_vma=False,
    )
```

```python
import functools

import jax
import jax.numpy as jnp
from jax import lax
from jax.experimental import pallas as pl
from jax.experimental.pallas import tpu as pltpu
from jax.sharding import PartitionSpec as P

NSI = 10
NAPP = 2
MESH = pl.DeviceIdType.MESH
F32 = jnp.float32
BF16 = jnp.bfloat16


def dot(a, b):
    return lax.dot_general(a, b, (((1,), (0,)), ((), ())), preferred_element_type=F32)


def dot_nt(a, b):
    return lax.dot_general(a, b, (((1,), (1,)), ((), ())), preferred_element_type=F32)


def dot_tn(a, b):
    return lax.dot_general(a, b, (((0,), (0,)), ((), ())), preferred_element_type=F32)


def split(x):
    hi = x.astype(BF16)
    return hi, (x - hi.astype(F32)).astype(BF16)


def as_lhs(pair):
    return jnp.concatenate(pair, axis=1)


def as_rhs(pair):
    row = jnp.concatenate(pair, axis=1)
    return jnp.concatenate((row, row), axis=0)


def mm(lhs_pair, rhs_pair):
    out = dot(as_lhs(lhs_pair), as_rhs(rhs_pair))
    width = out.shape[1] // 2
    return out[:, :width] + out[:, width:]


def kernel(
    steps, sites, parts, phys, owned,
    lc, rc, cs, cb, lseed, rseed, src, onsite, shift,
    left_new, right_new,
    hold_l, lrecv, lsend, rrecv, psend, terms, lct, site, bond, ys, zs, env_r, env_n,
    gsend, grecv, usend, urecv, fsend, frecv, fall, tns, tnr, trs, trr,
    s_ls, s_lr, s_ps, s_pr, s_gs, s_gr, s_us, s_ur, s_fs, s_fr, s_tns, s_tnr, s_trs, s_trr,
):
    j = lax.axis_index("site")
    me = lax.axis_index("sec")
    after, before = lax.rem(j + 1, sites), lax.rem(j + sites - 1, sites)
    off = me * owned
    width = lc.shape[-1]
    sectors = parts * owned

    def sec(d):
        return lax.rem(me + d, parts)

    def copy(a, b, ss, rs, to_site, to_sec):
        return pltpu.make_async_remote_copy(
            src_ref=a, dst_ref=b, send_sem=ss, recv_sem=rs,
            device_id={"site": to_site, "sec": to_sec}, device_id_type=MESH,
        )

    def c_seed(d):
        return copy(lseed.at[0], lrecv.at[0, me], s_ls.at[steps, d], s_lr.at[0, me], j, sec(d))

    def c_left(t, d):
        return copy(lsend.at[t], lrecv.at[t + 1, me], s_ls.at[t, d], s_lr.at[t + 1, me], after, sec(d))

    def c_right(t, d):
        return copy(psend.at[t, d], rrecv.at[t, me], s_ps.at[t, d], s_pr.at[t, me], before, sec(d))

    def c_tn(d):
        return copy(tns, tnr.at[me], s_tns.at[d], s_tnr.at[me], j, sec(d))

    def c_tr(d):
        return copy(trs, trr.at[me], s_trs.at[d], s_trr.at[me], before, sec(d))

    def c_gram(d):
        return copy(gsend.at[d], grecv.at[me], s_gs.at[d], s_gr.at[me], j, sec(d))

    def c_unit():
        return copy(usend, urecv, s_us.at[0], s_ur.at[0], after, me)

    def c_factor(d):
        return copy(fsend, frecv.at[me], s_fs.at[d], s_fr.at[me], j, sec(d))

    def got(ref, sem):
        copy(ref, ref, s_us.at[0], sem, after, me).wait_recv()

    barrier = pltpu.get_barrier_semaphore()
    for d in range(parts):
        for where in (after, before) if d == 0 else (after, before, j):
            pl.semaphore_signal(
                barrier, inc=1, device_id={"site": where, "sec": sec(d)}, device_id_type=MESH
            )
    pl.semaphore_wait(barrier, 3 * parts - 1)

    for d in range(1, parts):
        c_seed(d).start()

    sources = [[src[0, s, off + k] for k in range(owned)] for s in range(phys)]

    def gathered(target, i):
        want = target * owned + i
        total = None
        for s in range(phys):
            hit, at = jnp.int32(0), jnp.int32(0)
            for k in range(owned):
                same = (sources[s][k] == want).astype(jnp.int32)
                hit, at = hit + same, at + same * k
            term = terms[s * owned + at] * hit.astype(F32)
            total = term if total is None else total + term
        return total

    for k in range(owned):
        for s in range(phys):
            lct[k, :, s * width : (s + 1) * width] = lc[0, s, k].T
    for k in range(owned):
        env_r[k] = rseed[0, k]
        hold_l[off + k] = lseed[0, k]
    def seed_arrival():
        for d in range(1, parts):
            a = sec(d)
            got(lrecv.at[0, a], s_lr.at[0, a])
            for k in range(owned):
                hold_l[a * owned + k] = lrecv[0, a, k]

    def left_arrival(t):
        for d in range(parts):
            a = sec(d)
            got(lrecv.at[t, a], s_lr.at[t, a])
            for k in range(owned):
                hold_l[a * owned + k] = lrecv[t, a, k]

    def right_arrival(t):
        for d in range(parts):
            a = sec(d)
            got(rrecv.at[t, a], s_pr.at[t, a])
        for k in range(owned):
            total = rrecv[t, 0, k].astype(F32)
            for a in range(1, parts):
                total = total + rrecv[t, a, k].astype(F32)
            env_r[k] = total.astype(BF16)

    def turn(t, carry):
        @pl.when(t > 0)
        def _():
            right_arrival(t - 1)

        for k in range(owned):
            stack = jnp.concatenate([rc[0, s, k] for s in range(phys)], axis=0)
            prod = dot(stack, env_r[k]).astype(BF16)
            for s in range(phys):
                terms[s * owned + k] = dot_nt(prod[s * width : (s + 1) * width], rc[0, s, k])
        for d in reversed(range(parts)):
            for i in range(owned):
                psend[t, d, i] = gathered(sec(d), i).astype(BF16)
            c_right(t, d).start()

        @pl.when(t == 0)
        def _():
            seed_arrival()

        @pl.when(t > 0)
        def _():
            left_arrival(t)

        for k in range(owned):
            prods = [
                dot(hold_l[sources[s][k]], lc[0, s, k]).astype(BF16) for s in range(phys)
            ]
            lsend[t, k] = dot(lct[k], jnp.concatenate(prods, axis=0)).astype(BF16)
        for d in reversed(range(parts)):
            c_left(t, d).start()

        return carry

    lax.fori_loop(0, steps, turn, 0)

    rows = lax.broadcasted_iota(jnp.int32, (width, width), 0)
    cols = lax.broadcasted_iota(jnp.int32, (width, width), 1)
    diagonal = (rows == cols).astype(F32)

    def traces(blocks):
        total = None
        for block in blocks:
            total = block.astype(F32) if total is None else total + block.astype(F32)
        return jnp.sum((total * diagonal).reshape(width // 8, 8, width), axis=0)

    tns[...] = traces([lsend[steps - 1, k] for k in range(owned)])
    for d in range(1, parts):
        c_tn(d).start()
    trs[...] = traces([psend[steps - 1, d, i] for d in range(parts) for i in range(owned)])
    for d in range(parts):
        c_tr(d).start()

    def scale_of(total):
        return (sectors * width) / jnp.sum(total, axis=(0, 1), keepdims=True)

    total = tns[...]
    for d in range(1, parts):
        a = sec(d)
        got(tnr.at[a], s_tnr.at[a])
        total = total + tnr[a]
    scale = scale_of(total)
    for k in range(owned):
        env_n[k] = (lsend[steps - 1, k].astype(F32) * scale).astype(BF16)

    left_arrival(steps)
    scale = scale_of(traces([hold_l[m] for m in range(sectors)]))
    for m in range(sectors):
        hold_l[m] = (hold_l[m].astype(F32) * scale).astype(BF16)

    right_arrival(steps - 1)
    for a in range(parts):
        got(trr.at[a], s_trr.at[a])
    total = trr[0]
    for a in range(1, parts):
        total = total + trr[a]
    scale = scale_of(total)
    for k in range(owned):
        env_r[k] = (env_r[k].astype(F32) * scale).astype(BF16)

    for k in range(owned):
        for s in range(phys):
            site[k, s * width : (s + 1) * width] = cs[0, s, k]
        bond[k] = cb[0, k]
    for repeat in range(NAPP):
        for k in range(owned):
            halves = [
                dot(hold_l[sources[s][k]], site[k, s * width : (s + 1) * width]).astype(BF16)
                for s in range(phys)
            ]
            whole = dot(jnp.concatenate(halves, axis=0), env_r[k])
            for s in range(phys):
                part = slice(s * width, (s + 1) * width)
                site[k, part] = (whole[part] + onsite[0, s] * site[k, part].astype(F32)).astype(BF16)

    for k in range(owned):
        for s in range(phys):
            block = site[k, s * width : (s + 1) * width]
            terms[s * owned + k] = dot_nt(block, block)
    for d in range(parts - 1, -1, -1):
        for i in range(owned):
            gsend[d, i] = gathered(sec(d), i)
        if d > 0:
            c_gram(d).start()

    for repeat in range(NAPP):
        for k in range(owned):
            half = dot(env_n[k], bond[k]).astype(BF16)
            bond[k] = (dot(half, env_r[k]) + shift[0] * bond[k].astype(F32)).astype(BF16)

    def inverse_roots(grams):
        norms = []
        for i, gram in enumerate(grams):
            norm = jnp.sqrt(jnp.sum(gram * gram, axis=(0, 1), keepdims=True))
            norms.append(norm)
            upper = gram / norm
            middle = 1.5 * diagonal - 0.5 * upper
            ys[i] = mm(split(upper), split(middle))
            zs[i] = middle

        def body(n, carry):
            uppers = [split(ys[i]) for i in range(len(grams))]
            lowers = [split(zs[i]) for i in range(len(grams))]
            middles = [
                split(1.5 * diagonal - 0.5 * mm(z, y)) for z, y in zip(lowers, uppers)
            ]
            for i in range(len(grams)):
                ys[i] = mm(uppers[i], middles[i])
                zs[i] = mm(middles[i], lowers[i])
            return carry

        lax.fori_loop(0, NSI - 2, body, 0)
        for i in range(len(grams)):
            lower = split(zs[i])
            middle = split(1.5 * diagonal - 0.5 * mm(lower, split(ys[i])))
            zs[i] = mm(middle, lower) / jnp.sqrt(norms[i])

    inverse_roots(
        [dot_tn(bond[k], bond[k]) for k in range(owned)]
        + [dot_tn(site[k], site[k]) for k in range(owned)]
    )
    factors = []
    for k in range(owned):
        hi, lo = split(zs[k])
        unit_t = dot_nt(hi, bond[k]) + dot_nt(lo, bond[k])
        usend[k] = unit_t.astype(BF16)
        factors.append(mm(split(zs[owned + k]), split(unit_t)).astype(BF16))
    c_unit().start()

    for d in range(1, parts):
        a = sec(d)
        got(grecv.at[a], s_gr.at[a])
    grams = []
    for i in range(owned):
        total = gsend[0, i]
        for d in range(1, parts):
            total = total + grecv[sec(d), i]
        grams.append(total)
    inverse_roots(grams)
    got(urecv, s_ur.at[0])
    for i in range(owned):
        hi, lo = split(zs[i])
        fsend[i] = (dot(urecv[i], hi) + dot(urecv[i], lo)).astype(BF16)
    for d in range(1, parts):
        c_factor(d).start()

    for k in range(owned):
        whole = dot(site[k], factors[k]).astype(BF16)
        for s in range(phys):
            left_new[0, s, k] = whole[s * width : (s + 1) * width]
    for i in range(owned):
        fall[off + i] = fsend[i]
    for d in range(1, parts):
        a = sec(d)
        got(frecv.at[a], s_fr.at[a])
        for i in range(owned):
            fall[a * owned + i] = frecv[a, i]
    for k in range(owned):
        for s in range(phys):
            block = site[k, s * width : (s + 1) * width]
            right_new[0, s, k] = dot(fall[sources[s][k]], block).astype(BF16)

    def drain(t, carry):
        for d in range(parts):
            c_left(t, d).wait_send()
            c_right(t, d).wait_send()
        return carry

    lax.fori_loop(0, steps, drain, 0)
    for d in range(parts):
        c_tr(d).wait_send()
    for d in range(1, parts):
        for c in (c_seed, c_tn, c_gram, c_factor):
            c(d).wait_send()
    c_unit().wait_send()


def per_device(lc, rc, cs, cb, lseed, rseed, src, onsite, shift):
    sites, parts = lax.axis_size("site"), lax.axis_size("sec")
    steps = sites // 4
    _, phys, owned, width, _ = lc.shape
    sectors = parts * owned
    block = (width, width)
    most = 2 * owned

    def vm(*shape, dtype=BF16):
        return pltpu.VMEM(shape, dtype)

    def dma(*shape):
        return pltpu.SemaphoreType.DMA(shape)

    in_vmem = pl.BlockSpec(memory_space=pltpu.VMEM)
    in_smem = pl.BlockSpec(memory_space=pltpu.SMEM)
    shape = jax.ShapeDtypeStruct(cs.shape, BF16)
    return pl.pallas_call(
        functools.partial(kernel, steps, sites, parts, phys, owned),
        out_shape=(shape, shape),
        in_specs=[in_vmem] * 6 + [in_smem] * 3,
        out_specs=(in_vmem, in_vmem),
        scratch_shapes=[
            vm(sectors, *block),
            vm(steps + 1, parts, owned, *block),
            vm(steps, owned, *block),
            vm(steps, parts, owned, *block),
            vm(steps, parts, owned, *block),
            vm(phys * owned, *block, dtype=F32),
            vm(owned, width, phys * width),
            vm(owned, phys * width, width),
            vm(owned, *block),
            vm(most, *block, dtype=F32),
            vm(most, *block, dtype=F32),
            vm(owned, *block),
            vm(owned, *block),
            vm(parts, owned, *block, dtype=F32),
            vm(parts, owned, *block, dtype=F32),
            vm(owned, *block),
            vm(owned, *block),
            vm(owned, *block),
            vm(parts, owned, *block),
            vm(sectors, *block),
            vm(8, width, dtype=F32),
            vm(parts, 8, width, dtype=F32),
            vm(8, width, dtype=F32),
            vm(parts, 8, width, dtype=F32),
            dma(steps + 1, parts), dma(steps + 1, parts),
            dma(steps, parts), dma(steps, parts),
            dma(parts), dma(parts),
            dma(1), dma(1),
            dma(parts), dma(parts),
            dma(parts), dma(parts),
            dma(parts), dma(parts),
        ],
        compiler_params=pltpu.CompilerParams(
            collective_id=0, has_side_effects=True, vmem_limit_bytes=60 * 1024 * 1024
        ),
    )(lc, rc, cs, cb, lseed, rseed, src, onsite, shift)


def solution(mesh):
    tensor = P("site", None, "sec", None, None)
    blocks = P("site", "sec", None, None)
    return jax.shard_map(
        per_device,
        mesh=mesh,
        in_specs=(tensor, tensor, tensor, blocks, blocks, blocks,
                  P("site", None, None), P("site", None), P("site")),
        out_specs=(tensor, tensor),
        check_vma=False,
    )
```

```python
import functools

import jax
import jax.numpy as jnp
from jax import lax
from jax.experimental import pallas as pl
from jax.experimental.pallas import tpu as pltpu
from jax.sharding import PartitionSpec as P

NSI = 10
NAPP = 2
MESH = pl.DeviceIdType.MESH
F32 = jnp.float32
BF16 = jnp.bfloat16


def dot(a, b):
    return lax.dot_general(a, b, (((1,), (0,)), ((), ())), preferred_element_type=F32)


def dot_nt(a, b):
    return lax.dot_general(a, b, (((1,), (1,)), ((), ())), preferred_element_type=F32)


def dot_tn(a, b):
    return lax.dot_general(a, b, (((0,), (0,)), ((), ())), preferred_element_type=F32)


def split(x):
    hi = x.astype(BF16)
    return hi, (x - hi.astype(F32)).astype(BF16)


def as_lhs(pair):
    return jnp.concatenate(pair, axis=1)


def as_rhs(pair):
    row = jnp.concatenate(pair, axis=1)
    return jnp.concatenate((row, row), axis=0)


def mm(lhs_pair, rhs_pair):
    out = dot(as_lhs(lhs_pair), as_rhs(rhs_pair))
    width = out.shape[1] // 2
    return out[:, :width] + out[:, width:]


def kernel(
    steps, sites, parts, phys, owned,
    lc, rc, cs, cb, lseed, rseed, src, onsite, shift,
    site, fac, fall,
    hold_l, lrecv, lsend, rrecv, psend, terms, lct, bond, ys, zs, env_r, env_n,
    gsend, grecv, usend, urecv, fsend, frecv, tns, tnr, trs, trr,
    s_ls, s_lr, s_ps, s_pr, s_gs, s_gr, s_us, s_ur, s_fs, s_fr, s_tns, s_tnr, s_trs, s_trr,
):
    j = lax.axis_index("site")
    me = lax.axis_index("sec")
    after, before = lax.rem(j + 1, sites), lax.rem(j + sites - 1, sites)
    off = me * owned
    width = lc.shape[-1]
    sectors = parts * owned

    def sec(d):
        return lax.rem(me + d, parts)

    def copy(a, b, ss, rs, to_site, to_sec):
        return pltpu.make_async_remote_copy(
            src_ref=a, dst_ref=b, send_sem=ss, recv_sem=rs,
            device_id={"site": to_site, "sec": to_sec}, device_id_type=MESH,
        )

    def c_seed(d):
        return copy(lseed.at[0], lrecv.at[0, me], s_ls.at[steps, d], s_lr.at[0, me], j, sec(d))

    def c_left(t, d):
        return copy(lsend.at[t], lrecv.at[t + 1, me], s_ls.at[t, d], s_lr.at[t + 1, me], after, sec(d))

    def c_right(t, d):
        return copy(psend.at[t, d], rrecv.at[t, me], s_ps.at[t, d], s_pr.at[t, me], before, sec(d))

    def c_tn(d):
        return copy(tns, tnr.at[me], s_tns.at[d], s_tnr.at[me], j, sec(d))

    def c_tr(d):
        return copy(trs, trr.at[me], s_trs.at[d], s_trr.at[me], before, sec(d))

    def c_gram(d):
        return copy(gsend.at[d], grecv.at[me], s_gs.at[d], s_gr.at[me], j, sec(d))

    def c_unit():
        return copy(usend, urecv, s_us.at[0], s_ur.at[0], after, me)

    def c_factor(d):
        return copy(fsend, frecv.at[me], s_fs.at[d], s_fr.at[me], j, sec(d))

    def got(ref, sem):
        copy(ref, ref, s_us.at[0], sem, after, me).wait_recv()

    barrier = pltpu.get_barrier_semaphore()
    for d in range(parts):
        for where in (after, before) if d == 0 else (after, before, j):
            pl.semaphore_signal(
                barrier, inc=1, device_id={"site": where, "sec": sec(d)}, device_id_type=MESH
            )
    pl.semaphore_wait(barrier, 3 * parts - 1)

    for d in range(1, parts):
        c_seed(d).start()

    sources = [[src[0, s, off + k] for k in range(owned)] for s in range(phys)]

    def gathered(target, i):
        want = target * owned + i
        total = None
        for s in range(phys):
            hit, at = jnp.int32(0), jnp.int32(0)
            for k in range(owned):
                same = (sources[s][k] == want).astype(jnp.int32)
                hit, at = hit + same, at + same * k
            term = terms[s * owned + at] * hit.astype(F32)
            total = term if total is None else total + term
        return total

    for k in range(owned):
        for s in range(phys):
            lct[k, :, s * width : (s + 1) * width] = lc[0, s, k].T
    for k in range(owned):
        env_r[k] = rseed[0, k]
        hold_l[off + k] = lseed[0, k]
    def seed_arrival():
        for d in range(1, parts):
            a = sec(d)
            got(lrecv.at[0, a], s_lr.at[0, a])
            for k in range(owned):
                hold_l[a * owned + k] = lrecv[0, a, k]

    def left_arrival(t):
        for d in range(parts):
            a = sec(d)
            got(lrecv.at[t, a], s_lr.at[t, a])
            for k in range(owned):
                hold_l[a * owned + k] = lrecv[t, a, k]

    def right_arrival(t):
        for d in range(parts):
            a = sec(d)
            got(rrecv.at[t, a], s_pr.at[t, a])
        for k in range(owned):
            total = rrecv[t, 0, k].astype(F32)
            for a in range(1, parts):
                total = total + rrecv[t, a, k].astype(F32)
            env_r[k] = total.astype(BF16)

    def turn(t, carry):
        @pl.when(t > 0)
        def _():
            right_arrival(t - 1)

        for k in range(owned):
            stack = jnp.concatenate([rc[0, s, k] for s in range(phys)], axis=0)
            prod = dot(stack, env_r[k]).astype(BF16)
            for s in range(phys):
                terms[s * owned + k] = dot_nt(prod[s * width : (s + 1) * width], rc[0, s, k])
        for d in range(parts):
            for i in range(owned):
                psend[t, d, i] = gathered(sec(d), i).astype(BF16)
            c_right(t, d).start()

        @pl.when(t == 0)
        def _():
            seed_arrival()

        @pl.when(t > 0)
        def _():
            left_arrival(t)

        for k in range(owned):
            prods = [
                dot(hold_l[sources[s][k]], lc[0, s, k]).astype(BF16) for s in range(phys)
            ]
            lsend[t, k] = dot(lct[k], jnp.concatenate(prods, axis=0)).astype(BF16)
        for d in range(parts):
            c_left(t, d).start()

        return carry

    lax.fori_loop(0, steps, turn, 0)

    rows = lax.broadcasted_iota(jnp.int32, (width, width), 0)
    cols = lax.broadcasted_iota(jnp.int32, (width, width), 1)
    diagonal = (rows == cols).astype(F32)

    def traces(blocks):
        total = None
        for block in blocks:
            total = block.astype(F32) if total is None else total + block.astype(F32)
        return jnp.sum((total * diagonal).reshape(width // 8, 8, width), axis=0)

    tns[...] = traces([lsend[steps - 1, k] for k in range(owned)])
    for d in range(1, parts):
        c_tn(d).start()
    trs[...] = traces([psend[steps - 1, d, i] for d in range(parts) for i in range(owned)])
    for d in range(parts):
        c_tr(d).start()

    def scale_of(total):
        return (sectors * width) / jnp.sum(total, axis=(0, 1), keepdims=True)

    total = tns[...]
    for d in range(1, parts):
        a = sec(d)
        got(tnr.at[a], s_tnr.at[a])
        total = total + tnr[a]
    scale = scale_of(total)
    for k in range(owned):
        env_n[k] = (lsend[steps - 1, k].astype(F32) * scale).astype(BF16)

    left_arrival(steps)
    scale = scale_of(traces([hold_l[m] for m in range(sectors)]))
    for m in range(sectors):
        hold_l[m] = (hold_l[m].astype(F32) * scale).astype(BF16)

    right_arrival(steps - 1)
    for a in range(parts):
        got(trr.at[a], s_trr.at[a])
    total = trr[0]
    for a in range(1, parts):
        total = total + trr[a]
    scale = scale_of(total)
    for k in range(owned):
        env_r[k] = (env_r[k].astype(F32) * scale).astype(BF16)

    for k in range(owned):
        for s in range(phys):
            site[k, s * width : (s + 1) * width] = cs[0, s, k]
        bond[k] = cb[0, k]
    for repeat in range(NAPP):
        for k in range(owned):
            halves = [
                dot(hold_l[sources[s][k]], site[k, s * width : (s + 1) * width]).astype(BF16)
                for s in range(phys)
            ]
            whole = dot(jnp.concatenate(halves, axis=0), env_r[k])
            for s in range(phys):
                part = slice(s * width, (s + 1) * width)
                site[k, part] = (whole[part] + onsite[0, s] * site[k, part].astype(F32)).astype(BF16)

    for k in range(owned):
        for s in range(phys):
            block = site[k, s * width : (s + 1) * width]
            terms[s * owned + k] = dot_nt(block, block)
    for d in range(parts - 1, -1, -1):
        for i in range(owned):
            gsend[d, i] = gathered(sec(d), i)
        if d > 0:
            c_gram(d).start()

    for repeat in range(NAPP):
        for k in range(owned):
            half = dot(env_n[k], bond[k]).astype(BF16)
            bond[k] = (dot(half, env_r[k]) + shift[0] * bond[k].astype(F32)).astype(BF16)

    def inverse_roots(grams):
        norms = []
        for i, gram in enumerate(grams):
            norm = jnp.sqrt(jnp.sum(gram * gram, axis=(0, 1), keepdims=True))
            norms.append(norm)
            upper = gram / norm
            middle = 1.5 * diagonal - 0.5 * upper
            ys[i] = mm(split(upper), split(middle))
            zs[i] = middle

        def body(n, carry):
            uppers = [split(ys[i]) for i in range(len(grams))]
            lowers = [split(zs[i]) for i in range(len(grams))]
            middles = [
                split(1.5 * diagonal - 0.5 * mm(z, y)) for z, y in zip(lowers, uppers)
            ]
            for i in range(len(grams)):
                ys[i] = mm(uppers[i], middles[i])
                zs[i] = mm(middles[i], lowers[i])
            return carry

        lax.fori_loop(0, NSI - 2, body, 0)
        for i in range(len(grams)):
            lower = split(zs[i])
            middle = split(1.5 * diagonal - 0.5 * mm(lower, split(ys[i])))
            zs[i] = mm(middle, lower) / jnp.sqrt(norms[i])

    inverse_roots(
        [dot_tn(bond[k], bond[k]) for k in range(owned)]
        + [dot_tn(site[k], site[k]) for k in range(owned)]
    )
    for k in range(owned):
        hi, lo = split(zs[k])
        unit_t = dot_nt(hi, bond[k]) + dot_nt(lo, bond[k])
        usend[k] = unit_t.astype(BF16)
        fac[k] = mm(split(zs[owned + k]), split(unit_t)).astype(BF16)
    c_unit().start()

    for d in range(1, parts):
        a = sec(d)
        got(grecv.at[a], s_gr.at[a])
    grams = []
    for i in range(owned):
        total = gsend[0, i]
        for d in range(1, parts):
            total = total + grecv[sec(d), i]
        grams.append(total)
    inverse_roots(grams)
    got(urecv, s_ur.at[0])
    for i in range(owned):
        hi, lo = split(zs[i])
        fsend[i] = (dot(urecv[i], hi) + dot(urecv[i], lo)).astype(BF16)
    for d in range(1, parts):
        c_factor(d).start()

    for i in range(owned):
        fall[off + i] = fsend[i]
    for d in range(1, parts):
        a = sec(d)
        got(frecv.at[a], s_fr.at[a])
        for i in range(owned):
            fall[a * owned + i] = frecv[a, i]
    def drain(t, carry):
        for d in range(parts):
            c_left(t, d).wait_send()
            c_right(t, d).wait_send()
        return carry

    lax.fori_loop(0, steps, drain, 0)
    for d in range(parts):
        c_tr(d).wait_send()
    for d in range(1, parts):
        for c in (c_seed, c_tn, c_gram, c_factor):
            c(d).wait_send()
    c_unit().wait_send()


def finish(phys, owned, site, fac, fall, src, left_new, right_new):
    off = lax.axis_index("sec") * owned
    width = fac.shape[-1]
    for k in range(owned):
        whole = dot(site[k], fac[k]).astype(BF16)
        for s in range(phys):
            part = slice(s * width, (s + 1) * width)
            left_new[0, s, k] = whole[part]
            right_new[0, s, k] = dot(fall[src[0, s, off + k]], site[k, part]).astype(BF16)


def per_device(lc, rc, cs, cb, lseed, rseed, src, onsite, shift):
    sites, parts = lax.axis_size("site"), lax.axis_size("sec")
    steps = sites // 4
    _, phys, owned, width, _ = lc.shape
    sectors = parts * owned
    block = (width, width)
    most = 2 * owned

    def vm(*shape, dtype=BF16):
        return pltpu.VMEM(shape, dtype)

    def dma(*shape):
        return pltpu.SemaphoreType.DMA(shape)

    in_vmem = pl.BlockSpec(memory_space=pltpu.VMEM)
    in_smem = pl.BlockSpec(memory_space=pltpu.SMEM)
    shape = jax.ShapeDtypeStruct(cs.shape, BF16)
    site, fac, fall = pl.pallas_call(
        functools.partial(kernel, steps, sites, parts, phys, owned),
        out_shape=(
            jax.ShapeDtypeStruct((owned, phys * width, width), BF16),
            jax.ShapeDtypeStruct((owned, width, width), BF16),
            jax.ShapeDtypeStruct((sectors, width, width), BF16),
        ),
        in_specs=[in_vmem] * 6 + [in_smem] * 3,
        out_specs=(in_vmem,) * 3,
        scratch_shapes=[
            vm(sectors, *block),
            vm(steps + 1, parts, owned, *block),
            vm(steps, owned, *block),
            vm(steps, parts, owned, *block),
            vm(steps, parts, owned, *block),
            vm(phys * owned, *block, dtype=F32),
            vm(owned, width, phys * width),
            vm(owned, *block),
            vm(most, *block, dtype=F32),
            vm(most, *block, dtype=F32),
            vm(owned, *block),
            vm(owned, *block),
            vm(parts, owned, *block, dtype=F32),
            vm(parts, owned, *block, dtype=F32),
            vm(owned, *block),
            vm(owned, *block),
            vm(owned, *block),
            vm(parts, owned, *block),
            vm(8, width, dtype=F32),
            vm(parts, 8, width, dtype=F32),
            vm(8, width, dtype=F32),
            vm(parts, 8, width, dtype=F32),
            dma(steps + 1, parts), dma(steps + 1, parts),
            dma(steps, parts), dma(steps, parts),
            dma(parts), dma(parts),
            dma(1), dma(1),
            dma(parts), dma(parts),
            dma(parts), dma(parts),
            dma(parts), dma(parts),
        ],
        compiler_params=pltpu.CompilerParams(
            collective_id=0, has_side_effects=True, vmem_limit_bytes=32 * 1024 * 1024
        ),
    )(lc, rc, cs, cb, lseed, rseed, src, onsite, shift)
    return pl.pallas_call(
        functools.partial(finish, phys, owned),
        out_shape=(shape, shape),
        in_specs=[in_vmem] * 3 + [in_smem],
        out_specs=(in_vmem, in_vmem),
        compiler_params=pltpu.CompilerParams(vmem_limit_bytes=16 * 1024 * 1024),
    )(site, fac, fall, src)


def solution(mesh):
    tensor = P("site", None, "sec", None, None)
    blocks = P("site", "sec", None, None)
    return jax.shard_map(
        per_device,
        mesh=mesh,
        in_specs=(tensor, tensor, tensor, blocks, blocks, blocks,
                  P("site", None, None), P("site", None), P("site")),
        out_specs=(tensor, tensor),
        check_vma=False,
    )
```
